8 devices in a mesh: part: 1 (over z), tp: 2 (over y), dp: 4 (over x, core).
Axes of the slice: x: 2, y: 2, z: 1, core: 2. Of those that a mesh axis runs over, the one named last changes fastest.
Arguments:
- features: bfloat16 [256, 196, 768], P(('part', 'tp', 'dp'))
- img_pos: int32 [48, 768], P(('part', 'dp'))
- token_ids: int32 [48, 768], P(('part', 'dp'))
- embedding: bfloat16 [50304, 1024], P('tp')
- conn_ln_w: bfloat16 [3072], replicated
- conn_ln_b: bfloat16 [3072], replicated
- conn_w1: bfloat16 [3072, 8192], replicated
- conn_b1: bfloat16 [8192], replicated
- conn_w2: bfloat16 [4096, 1024], replicated
- conn_b2: bfloat16 [1024], replicated
- ln_w: bfloat16 [1024], replicated
- w_q: bfloat16 [1024, 16, 64], P(None, 'tp')
- w_k: bfloat16 [1024, 16, 64], P(None, 'tp')
- w_v: bfloat16 [1024, 16, 64], P(None, 'tp')
- w_o: bfloat16 [16, 64, 1024], P('tp')
- w_gate: bfloat16 [1024, 4096], P(None, 'tp')
- w_up: bfloat16 [1024, 4096], P(None, 'tp')
- w_down: bfloat16 [4096, 1024], P('tp')
Outputs:
- output: bfloat16 [48, 768, 1024], P(('part', 'dp'))
All inputs are finite; a program needn't handle non-finite values.
Results may differ from the reference program's by a relative error of at most 0.00932157.
Values are sent between devices in bfloat16 or wider.
A program may use at most 1 GiB of HBM per device.

```python
import jax
import jax.numpy as jnp
from jax import lax

VIS_WIDTH = 768
GRID_SIDE = 14
CONN_HIDDEN = 4096
D = 1024
HEADS = 16
KV_HEADS = 16
HEAD = 64
FF = 4096
VOCAB = 50304
SEQ_LEN = 768
BATCH = 48
NUM_TILES = 256
MAX_TILES = 12
QUERY_ROWS = 256

GRID_HALF = GRID_SIDE // 2
TILE_TOKENS = GRID_HALF * GRID_HALF
PATCHES = GRID_SIDE * GRID_SIDE
MERGED_WIDTH = 4 * VIS_WIDTH
GROUP_SIZE = HEADS // KV_HEADS
ROPE_THETA = 50000.0
CONN_EPS = 1e-6
LAYER_EPS = 1e-5


def draw_layout(key):
    key_full, key_slots, key_perm, key_offset, key_ids = jax.random.split(key, 5)
    slot_total = BATCH * (MAX_TILES - 1)
    req_order = jax.random.permutation(key_full, BATCH)
    slot_req = jnp.arange(slot_total) // (MAX_TILES - 1)
    priority = jax.random.permutation(key_slots, slot_total)
    priority = priority + slot_total * (slot_req == req_order[1]).astype(jnp.int32) - slot_total * (slot_req == req_order[0]).astype(jnp.int32)
    slot_rank = jnp.argsort(jnp.argsort(priority))
    chosen = (slot_rank < NUM_TILES - BATCH).astype(jnp.int32)
    tile_count = 1 + jnp.sum(chosen.reshape(BATCH, MAX_TILES - 1), axis=1)
    count_end = jnp.cumsum(tile_count)
    tile_index = jnp.arange(NUM_TILES)
    sorted_rows = jnp.sum((count_end[None, :] <= tile_index[:, None]).astype(jnp.int32), axis=1)
    tile_req = sorted_rows[jax.random.permutation(key_perm, NUM_TILES)]
    req_hot = (tile_req[:, None] == jnp.arange(BATCH)[None, :]).astype(jnp.int32)
    tile_rank = jnp.sum((jnp.cumsum(req_hot, axis=0) - req_hot) * req_hot, axis=1)
    rank_hot = (tile_rank[:, None] == jnp.arange(MAX_TILES)[None, :]).astype(jnp.int32)
    tile_of = jnp.sum(req_hot[:, :, None] * rank_hot[:, None, :] * tile_index[:, None, None], axis=0)
    image_len = tile_count * TILE_TOKENS
    offset = jax.random.randint(key_offset, (BATCH,), 0, SEQ_LEN - 7 - image_len)
    rel_pos = jnp.arange(SEQ_LEN)[None, :] - offset[:, None]
    inside = (rel_pos >= 0) & (rel_pos < image_len[:, None])
    rel_safe = jnp.clip(rel_pos, 0, MAX_TILES * TILE_TOKENS - 1)
    tile_here = jnp.take_along_axis(tile_of, rel_safe // TILE_TOKENS, axis=1)
    img_pos = jnp.where(inside, tile_here * TILE_TOKENS + rel_safe % TILE_TOKENS, -1).astype(jnp.int32)
    token_ids = jax.random.randint(key_ids, (BATCH, SEQ_LEN), 0, VOCAB)
    token_ids = token_ids.at[0, SEQ_LEN - 1].set(VOCAB - 1).at[0, SEQ_LEN - 2].set(0)
    return img_pos, token_ids.astype(jnp.int32)


def normal_draw(key, shape, scale):
    return (jax.random.normal(key, shape, jnp.float32) * scale).astype(jnp.bfloat16)


def setup_inputs(seed: int = 0, part: int = 0) -> dict:
    key_shared, key_part = jax.random.split(jax.random.key(seed))
    key_layout, key_feat = jax.random.split(jax.random.fold_in(key_part, part))
    img_pos, token_ids = draw_layout(key_layout)
    keys = jax.random.split(key_shared, 15)
    return {
        'features': normal_draw(key_feat, (NUM_TILES, PATCHES, VIS_WIDTH), 1.0),
        'img_pos': img_pos,
        'token_ids': token_ids,
        'embedding': normal_draw(keys[0], (VOCAB, D), 1.0),
        'conn_ln_w': (1.0 + 0.4 * jax.random.normal(keys[1], (MERGED_WIDTH,), jnp.float32)).astype(jnp.bfloat16),
        'conn_ln_b': normal_draw(keys[2], (MERGED_WIDTH,), 0.4),
        'conn_w1': normal_draw(keys[3], (MERGED_WIDTH, 2 * CONN_HIDDEN), MERGED_WIDTH ** -0.5),
        'conn_b1': normal_draw(keys[4], (2 * CONN_HIDDEN,), 0.5),
        'conn_w2': normal_draw(keys[5], (CONN_HIDDEN, D), CONN_HIDDEN ** -0.5),
        'conn_b2': normal_draw(keys[6], (D,), 0.5),
        'ln_w': (1.0 + 0.4 * jax.random.normal(keys[7], (D,), jnp.float32)).astype(jnp.bfloat16),
        'w_q': normal_draw(keys[8], (D, HEADS, HEAD), 3.0 * D ** -0.5),
        'w_k': normal_draw(keys[9], (D, KV_HEADS, HEAD), D ** -0.5),
        'w_v': normal_draw(keys[10], (D, KV_HEADS, HEAD), D ** -0.5),
        'w_o': normal_draw(keys[11], (HEADS, HEAD, D), (HEADS * HEAD) ** -0.5),
        'w_gate': normal_draw(keys[12], (D, FF), D ** -0.5),
        'w_up': normal_draw(keys[13], (D, FF), D ** -0.5),
        'w_down': normal_draw(keys[14], (FF, D), FF ** -0.5),
    }


def connector(tile_feats, conn_ln_w, conn_ln_b, conn_w1, conn_b1, conn_w2, conn_b2):
    merged = tile_feats.reshape(GRID_HALF, 2, GRID_HALF, 2, VIS_WIDTH).transpose(0, 2, 1, 3, 4)
    merged = merged.reshape(TILE_TOKENS, MERGED_WIDTH).astype(jnp.float32)
    centered = merged - jnp.mean(merged, axis=-1, keepdims=True)
    variance = jnp.mean(centered * centered, axis=-1, keepdims=True)
    normed = centered * lax.rsqrt(variance + CONN_EPS) * conn_ln_w.astype(jnp.float32) + conn_ln_b.astype(jnp.float32)
    hidden = jnp.dot(normed.astype(jnp.bfloat16), conn_w1, preferred_element_type=jnp.float32) + conn_b1.astype(jnp.float32)
    gated = jax.nn.silu(hidden[:, CONN_HIDDEN:]) * hidden[:, :CONN_HIDDEN]
    result = jnp.dot(gated.astype(jnp.bfloat16), conn_w2, preferred_element_type=jnp.float32) + conn_b2.astype(jnp.float32)
    return result.astype(jnp.bfloat16)


def rotate(vectors, cos_t, sin_t):
    pairs = vectors.reshape(vectors.shape[:-1] + (HEAD // 2, 2))
    real_part = pairs[..., 0]
    imag_part = pairs[..., 1]
    turned = jnp.stack([real_part * cos_t - imag_part * sin_t, imag_part * cos_t + real_part * sin_t], axis=-1)
    return turned.reshape(vectors.shape)


def decoder_layer(hidden, ln_w, w_q, w_k, w_v, w_o, w_gate, w_up, w_down):
    base = hidden.astype(jnp.float32)
    centered = base - jnp.mean(base, axis=-1, keepdims=True)
    variance = jnp.mean(centered * centered, axis=-1, keepdims=True)
    normed = (centered * lax.rsqrt(variance + LAYER_EPS) * ln_w.astype(jnp.float32)).astype(jnp.bfloat16)
    normed_wide = normed.astype(jnp.float32)
    positions = jnp.arange(SEQ_LEN, dtype=jnp.float32)
    inv_freq = ROPE_THETA ** (-jnp.arange(0, HEAD, 2, dtype=jnp.float32) / HEAD)
    angles = positions[:, None] * inv_freq[None, :]
    cos_t = jnp.cos(angles)[:, None, :]
    sin_t = jnp.sin(angles)[:, None, :]
    query = rotate(jnp.einsum('td,dhe->the', normed_wide, w_q.astype(jnp.float32)), cos_t, sin_t).astype(jnp.bfloat16)
    keys = rotate(jnp.einsum('td,dke->tke', normed_wide, w_k.astype(jnp.float32)), cos_t, sin_t).astype(jnp.bfloat16)
    values = jnp.einsum('td,dke->tke', normed_wide, w_v.astype(jnp.float32)).astype(jnp.bfloat16)
    query_grouped = query.reshape(SEQ_LEN, KV_HEADS, GROUP_SIZE, HEAD)
    keys_wide = keys.astype(jnp.float32)
    values_wide = values.astype(jnp.float32)
    scale = HEAD ** -0.5

    def block_attend(block_index):
        start = block_index * QUERY_ROWS
        query_block = lax.dynamic_slice_in_dim(query_grouped, start, QUERY_ROWS, axis=0).astype(jnp.float32)
        scores = jnp.einsum('qkge,ske->kgqs', query_block, keys_wide) * scale
        allowed = (start + jnp.arange(QUERY_ROWS))[:, None] >= jnp.arange(SEQ_LEN)[None, :]
        scores = jnp.where(allowed, scores, -jnp.inf)
        attn_probs = jax.nn.softmax(scores, axis=-1).astype(jnp.bfloat16).astype(jnp.float32)
        return jnp.einsum('kgqs,ske->qkge', attn_probs, values_wide).astype(jnp.bfloat16)

    attended = lax.map(block_attend, jnp.arange(SEQ_LEN // QUERY_ROWS)).reshape(SEQ_LEN, HEADS, HEAD)
    branch = jnp.einsum('the,hed->td', attended.astype(jnp.float32), w_o.astype(jnp.float32))
    gate = jnp.dot(normed, w_gate, preferred_element_type=jnp.float32)
    up_proj = jnp.dot(normed, w_up, preferred_element_type=jnp.float32)
    gated = (jax.nn.silu(gate) * up_proj).astype(jnp.bfloat16)
    mlp_out = jnp.dot(gated, w_down, preferred_element_type=jnp.float32)
    return (base + branch + mlp_out).astype(jnp.bfloat16)


def reference(features, img_pos, token_ids, embedding, conn_ln_w, conn_ln_b, conn_w1, conn_b1, conn_w2, conn_b2, ln_w, w_q, w_k, w_v, w_o, w_gate, w_up, w_down):
    image_rows = lax.map(lambda tile: connector(tile, conn_ln_w, conn_ln_b, conn_w1, conn_b1, conn_w2, conn_b2), features)
    image_rows = image_rows.reshape(NUM_TILES * TILE_TOKENS, D)

    def one_sequence(row_args):
        pos_row, id_row = row_args
        text_rows = jnp.take(embedding, id_row, axis=0)
        picked = jnp.take(image_rows, jnp.maximum(pos_row, 0), axis=0)
        hidden = jnp.where((pos_row >= 0)[:, None], picked, text_rows)
        return decoder_layer(hidden, ln_w, w_q, w_k, w_v, w_o, w_gate, w_up, w_down)

    return lax.map(one_sequence, (img_pos, token_ids))
```

```python
import math
import jax
import jax.numpy as jnp
from jax import lax
from jax.experimental import pallas as pl
from jax.experimental.pallas import tpu as pltpu
from jax.sharding import PartitionSpec as P

ROPE_THETA = 50000.0
CONN_EPS = 1e-6
LAYER_EPS = 1e-5
QUERY_ROWS = 256
LANES = 128
CHUNKS = (3, 2, 1)

IN_SPECS = (P(('part', 'tp', 'dp'), None, None), P(('part', 'dp'), None), P(('part', 'dp'), None), P('tp', None),
            P(None), P(None), P(None, None), P(None), P(None, None), P(None), P(None),
            P(None, 'tp', None), P(None, 'tp', None), P(None, 'tp', None), P('tp', None, None),
            P(None, 'tp'), P(None, 'tp'), P('tp', None))
OUT_SPEC = P(('part', 'dp'), None, None)
SWAP = [(0, 1), (1, 0)]


def normalize(values, epsilon):
    base = values.astype(jnp.float32)
    centered = base - jnp.mean(base, axis=-1, keepdims=True)
    variance = jnp.mean(centered * centered, axis=-1, keepdims=True)
    return centered * lax.rsqrt(variance + epsilon)


def connector(features, after, conn_ln_w, conn_ln_b, conn_w1, conn_b1, conn_w2, conn_b2):
    tiles, patches, vis_width = features.shape
    half = math.isqrt(patches) // 2
    merged = features.reshape(tiles, half, 2, half, 2, vis_width).transpose(0, 1, 3, 2, 4, 5)
    merged = lax.optimization_barrier(merged.reshape(tiles * half * half, 4 * vis_width))
    normed = (normalize(merged, CONN_EPS) * conn_ln_w.astype(jnp.float32) + conn_ln_b.astype(jnp.float32)).astype(jnp.bfloat16)
    normed, after = lax.optimization_barrier((normed, after))
    hidden = jnp.dot(normed, conn_w1, preferred_element_type=jnp.float32) + conn_b1.astype(jnp.float32)
    conn_hidden = conn_w2.shape[0]
    gated = (jax.nn.silu(hidden[:, conn_hidden:]) * hidden[:, :conn_hidden]).astype(jnp.bfloat16)
    rows = jnp.dot(gated, conn_w2, preferred_element_type=jnp.float32) + conn_b2.astype(jnp.float32)
    return rows.astype(jnp.bfloat16), after


def attention_kernel(head_dim, q_ref, k_ref, v_ref, cos_ref, sin_ref, out_ref):
    seq_len, width = q_ref.shape[1], q_ref.shape[2]
    cos_t, sin_t = cos_ref[...], sin_ref[...]
    lane = lax.broadcasted_iota(jnp.int32, (seq_len, width), 1)
    even = lane % 2 == 0

    def rotate(vectors):
        partner = jnp.where(even, pltpu.roll(vectors, width - 1, 1), pltpu.roll(vectors, 1, 1))
        return vectors * cos_t + partner * sin_t

    query = rotate(q_ref[0]).astype(jnp.bfloat16) * jnp.asarray(head_dim ** -0.5, jnp.bfloat16)
    keys = rotate(k_ref[0]).astype(jnp.bfloat16)
    values_t = v_ref[0].T.astype(jnp.bfloat16)
    heads = width // head_dim
    row = lax.broadcasted_iota(jnp.int32, (QUERY_ROWS, QUERY_ROWS), 0)
    column = lax.broadcasted_iota(jnp.int32, (QUERY_ROWS, QUERY_ROWS), 1)
    allowed = jnp.concatenate([row <= column] * heads, axis=1)
    out_lane = lax.broadcasted_iota(jnp.int32, (QUERY_ROWS, width), 1)
    masks = [(out_lane >= head * head_dim) & (out_lane < (head + 1) * head_dim) for head in range(heads)]
    out_row = lax.broadcasted_iota(jnp.int32, (width, QUERY_ROWS), 0)
    for start in range(0, seq_len, QUERY_ROWS):
        stop = start + QUERY_ROWS
        part = query[start:stop].astype(jnp.float32)
        block = jnp.concatenate([jnp.where(mine, part, 0.0) for mine in masks], axis=0).astype(jnp.bfloat16)
        scores = lax.dot_general(keys[:stop], block, (((1,), (1,)), ((), ())), preferred_element_type=jnp.float32)
        diagonal = jnp.where(allowed, scores[start:], -jnp.inf)
        scores = diagonal if start == 0 else jnp.concatenate([scores[:start], diagonal], axis=0)
        weights = jnp.exp(scores - jnp.max(scores, axis=0, keepdims=True))
        weights = (weights * (1.0 / jnp.sum(weights, axis=0, keepdims=True))).astype(jnp.bfloat16)
        product = lax.dot_general(values_t[:, :stop], weights, (((1,), (0,)), ((), ())), preferred_element_type=jnp.float32)
        result = product[:, :QUERY_ROWS]
        for head in range(1, heads):
            result = jnp.where(out_row >= head * head_dim, product[:, head * QUERY_ROWS:(head + 1) * QUERY_ROWS], result)
        result = result.T
        out_ref[0, start:stop, :] = result.astype(jnp.bfloat16)


def attention(qkv, cos_t, sin_t, head_dim):
    batch, seq_len, total = qkv.shape
    width = total // 3
    groups = width // LANES

    def spec(offset):
        return pl.BlockSpec((1, seq_len, LANES), lambda b, g: (b, 0, offset + g))

    table = pl.BlockSpec((seq_len, LANES), lambda b, g: (0, 0))

    def kernel(*refs):
        attention_kernel(head_dim, *refs)

    pairs = batch * width // head_dim * seq_len * seq_len
    return pl.pallas_call(
        kernel,
        name='attention',
        grid=(batch, groups),
        out_shape=jax.ShapeDtypeStruct((batch, seq_len, width), jnp.bfloat16),
        in_specs=[spec(0), spec(groups), spec(2 * groups), table, table],
        out_specs=spec(0),
        compiler_params=pltpu.CompilerParams(dimension_semantics=('parallel', 'parallel'), vmem_limit_bytes=48 * 1024 * 1024),
        cost_estimate=pl.CostEstimate(flops=pairs * head_dim * 4, bytes_accessed=batch * seq_len * width * 14, transcendentals=pairs),
    )(qkv, qkv, qkv, cos_t, sin_t)


def rope_tables(seq_len, head_dim):
    positions = jnp.arange(seq_len, dtype=jnp.float32)
    inv_freq = ROPE_THETA ** (-jnp.arange(0, head_dim, 2, dtype=jnp.float32) / head_dim)
    angles = positions[:, None] * inv_freq[None, :]
    copies = LANES // head_dim
    cos_t = jnp.tile(jnp.repeat(jnp.cos(angles), 2, axis=1), (1, copies))
    sign = jnp.where(jnp.arange(LANES) % 2 == 0, -1.0, 1.0).astype(jnp.float32)
    sin_t = jnp.tile(jnp.repeat(jnp.sin(angles), 2, axis=1), (1, copies)) * sign
    return lax.optimization_barrier((cos_t, sin_t))


def decoder_layer(hidden, ln_w, shards, cos_t, sin_t, head_dim):
    batch, seq_len, d_model = hidden.shape
    normed = (normalize(hidden, LAYER_EPS) * ln_w.astype(jnp.float32)).astype(jnp.bfloat16)
    normed = lax.optimization_barrier(normed.reshape(batch * seq_len, d_model))
    total = hidden.reshape(batch * seq_len, d_model).astype(jnp.float32)
    for w_qkv, w_gate, w_up, w_o, w_down in shards:
        qkv = jnp.dot(normed, w_qkv, preferred_element_type=jnp.float32)
        attended = attention(qkv.reshape(batch, seq_len, -1), cos_t, sin_t, head_dim)
        total = total + jnp.dot(attended.reshape(batch * seq_len, -1), w_o, preferred_element_type=jnp.float32)
        gate = jnp.dot(normed, w_gate, preferred_element_type=jnp.float32)
        up_proj = jnp.dot(normed, w_up, preferred_element_type=jnp.float32)
        gated = (jax.nn.silu(gate) * up_proj).astype(jnp.bfloat16)
        total = total + jnp.dot(gated, w_down, preferred_element_type=jnp.float32)
    return total.astype(jnp.bfloat16).reshape(batch, seq_len, d_model)


def part_from_peer(shard, copies):
    part = shard.shape[0] // copies
    mine = lax.dynamic_slice_in_dim(shard, lax.axis_index('dp') * part, part, axis=0)
    return lax.ppermute(mine, 'tp', SWAP)


def solution(mesh):
    dp = mesh.shape['dp']

    def local(features, img_pos, token_ids, embedding, conn_ln_w, conn_ln_b, conn_w1, conn_b1, conn_w2, conn_b2, ln_w, w_q, w_k, w_v, w_o, w_gate, w_up, w_down):
        d_model, heads, head_dim = w_q.shape
        width, ff = heads * head_dim, w_gate.shape[1]
        batch, seq_len = token_ids.shape
        tp = lax.axis_index('tp')
        vocab_rows = embedding.shape[0]

        w_in = jnp.concatenate([w_q.reshape(d_model, width), w_k.reshape(d_model, width), w_v.reshape(d_model, width), w_gate, w_up], axis=1)
        w_out = jnp.concatenate([w_o.reshape(width, d_model), w_down], axis=0)
        part_in, part_out = part_from_peer(w_in, dp), part_from_peer(w_out, dp)

        own_rows, peer_rows, first = [], [], 0
        for size in CHUNKS:
            own_rows.append(first + tp * size + jnp.arange(size))
            peer_rows.append(first + (1 - tp) * size + jnp.arange(size))
            first += 2 * size
        own_rows, peer_rows = jnp.concatenate(own_rows), jnp.concatenate(peer_rows)
        own_ids = jnp.take(token_ids, own_rows, axis=0) - tp * vocab_rows
        peer_ids = jnp.take(token_ids, peer_rows, axis=0) - tp * vocab_rows
        own_pos = jnp.take(img_pos, own_rows, axis=0)

        split = vocab_rows // 2
        lower, upper = lax.optimization_barrier((embedding[:split], embedding[split:]))

        def text_rows(ids):
            flat = ids.reshape(-1)
            low = jnp.take(lower, jnp.clip(flat, 0, split - 1), axis=0)
            high = jnp.take(upper, jnp.clip(flat - split, 0, vocab_rows - split - 1), axis=0)
            return jnp.where((flat < split)[:, None], low, high)

        sent = text_rows(peer_ids)
        features, sent, part_in, part_out = lax.optimization_barrier((features, sent, part_in, part_out))
        received = lax.ppermute(sent, 'tp', SWAP)
        conn_params = (conn_ln_w, conn_ln_b, conn_w1, conn_b1, conn_w2, conn_b2)
        tiles = features.shape[0] // 2
        rows_a, rest = connector(features[:tiles], features[tiles:], *conn_params)
        table_a = lax.all_gather(rows_a, ('tp', 'dp'), axis=0, tiled=True)
        rows_b, own_ids = connector(rest, own_ids, *conn_params)
        rows_b, own_ids, received, part_in, part_out = lax.optimization_barrier((rows_b, own_ids, received, part_in, part_out))
        table_b = lax.all_gather(rows_b, ('tp', 'dp'), axis=0, tiled=True)
        table_b, part_in, part_out = lax.optimization_barrier((table_b, part_in, part_out))
        peer_in = lax.all_gather(part_in, 'dp', axis=0, tiled=True)
        peer_out = lax.all_gather(part_out, 'dp', axis=0, tiled=True)
        shards = []
        for big_in, big_out in ((w_in, w_out), (peer_in, peer_out)):
            shards.append((big_in[:, :3 * width], big_in[:, 3 * width:3 * width + ff], big_in[:, 3 * width + ff:], big_out[:width], big_out[width:]))

        kept = text_rows(own_ids)
        half = rows_a.shape[0]
        flat_pos = jnp.maximum(own_pos, 0).reshape(-1)
        owner, offset = flat_pos // (2 * half), flat_pos % (2 * half)
        from_a = jnp.take(table_a, owner * half + jnp.minimum(offset, half - 1), axis=0)
        from_b = jnp.take(table_b, owner * half + jnp.maximum(offset - half, 0), axis=0)
        picked = jnp.where((offset < half)[:, None], from_a, from_b)
        owned = ((own_ids >= 0) & (own_ids < vocab_rows)).reshape(-1, 1)
        is_image = (own_pos >= 0).reshape(-1, 1)
        hidden = jnp.where(is_image, picked, jnp.where(owned, kept, received))
        hidden = lax.optimization_barrier(hidden).reshape(-1, seq_len, d_model)

        cos_t, sin_t = rope_tables(seq_len, head_dim)
        whole, first = jnp.zeros((batch, seq_len, d_model), hidden.dtype), 0
        for size in CHUNKS:
            piece = decoder_layer(hidden[first:first + size], ln_w, shards, cos_t, sin_t, head_dim)
            piece = lax.all_gather(piece, 'tp', axis=0, tiled=True)
            whole = lax.dynamic_update_slice_in_dim(whole, piece, 2 * first, axis=0)
            first += size
        return whole

    return jax.shard_map(local, mesh=mesh, in_specs=IN_SPECS, out_specs=OUT_SPEC, check_vma=False)
```
